32 devices in a mesh: tm: 16 (over z, x, core), freq: 2 (over y).
Axes of the slice: x: 2, y: 2, z: 4, core: 2. Of those that a mesh axis runs over, the one named last changes fastest.
Arguments:
- strengths: bfloat16 [2, 8, 256, 32768], P(None, 'freq', None, 'tm'), may hold values from -6 to 6
- sample_cell: int32 [32768], P('tm'), may hold values from 0 to 16383, as said below
- sample_frac: float32 [32768], P('tm'), may hold values from 0 to 1
Outputs:
- spectra: float32 [2, 8, 256, 4, 32, 128], P(None, None, 'tm', 'freq')
The draws below stay inside these ranges and needn't reach their ends.
Inputs may be any that keep to these rules, and one draw needn't show every extreme that they name: `sample_cell`: the samples of the i-th aligned block of 2048 samples lie in cells i * 1024 to (i + 1) * 1024 - 1; in every block the first sample lies in the first of these cells and the second sample in the last.
All inputs are finite; a program needn't handle non-finite values.
Results may differ from the reference program's by a relative error of at most 0.0037.
Values may be sent and summed in bfloat16 or wider, within the bound.
No kernel may reach another device: no remote copies, remote signals or barrier semaphores. Data moves between devices by JAX's collectives and lax.ppermute only.
A program may use at most 128 MiB of HBM per device.

```python
import math
import jax
import jax.numpy as jnp
from jax import lax

TAPS = 8
FGROUPS = 8
CHG = 256
GRID_DEV = 1024
SAMP_DEV = 2048
FFT_LO = 32
FFT_HI = 128
FFTLEN = 4096
SAMPLES = 32768
CELLS = 16384
FRAMES = 4


def draw_sample_cell(key, part):
    offsets = jax.random.randint(key, (SAMPLES,), 0, GRID_DEV)
    within = jnp.arange(SAMPLES) % SAMP_DEV
    offsets = jnp.where(within == 0, 0, jnp.where(within == 1, GRID_DEV - 1, offsets))
    blocks = jnp.arange(SAMPLES) // SAMP_DEV
    return (blocks * GRID_DEV + offsets).astype(jnp.int32)


def levels(rng, dims, cuts, least, largest):
    gain, own = 1.0, jax.random.fold_in(rng, 6)
    for dim, blocks in cuts:
        heights = jnp.exp(jax.random.uniform(jax.random.fold_in(own, dim), (blocks,), jnp.float32, least / len(cuts), largest / len(cuts)))
        gain = gain * jnp.repeat(heights, dims[dim] // blocks).reshape([-1 if axis == dim else 1 for axis in range(len(dims))])
    return gain


def scatter_about(key, dims, scale, reach, shards=(), dtype=jnp.bfloat16):
    factor_of = levels(key, dims, shards, -0.22, 0.18) if shards else 1.0
    drawn = jax.random.normal(key, dims, jnp.float32) * scale * factor_of
    return jnp.minimum(jnp.maximum(drawn, -reach), reach).astype(dtype)


def setup_inputs(seed: int = 0) -> dict:
    splits = jax.random.split(jax.random.key(seed), 4)
    return {
        "strengths": scatter_about(splits[0], (2, FGROUPS, CHG, SAMPLES), 1.0, 6.0, ((1, 2), (3, 16))),
        "sample_cell": draw_sample_cell(jax.random.fold_in(splits[3], 71), 0),
        "sample_frac": jnp.clip(1.0 * jax.random.uniform(splits[2], (SAMPLES,), jnp.float32) ** levels(splits[2], (SAMPLES,), ((0, 16),), -0.2, 0.2), 0.0, 1.0),
    }


sharpness = 0.3

def one_group(group_strengths, sample_cell, sample_frac):
    values = group_strengths.astype(jnp.float32)
    accumulated = jnp.zeros((2, CHG, CELLS), jnp.float32)
    for tap_index in range(TAPS):
        shifted = jnp.float32(tap_index) - float(TAPS // 2 - 1) - sample_frac
        weight_row = lax.optimization_barrier(jnp.exp(-sharpness * (shifted * shifted)).astype(jnp.bfloat16)).astype(jnp.float32)
        target = ((sample_cell + (tap_index - (TAPS // 2 - 1))) % CELLS).astype(jnp.int32)
        accumulated = accumulated.at[:, :, target].add(values * weight_row)
    rounded = lax.optimization_barrier(accumulated.astype(jnp.bfloat16)).astype(jnp.float32)
    framed = rounded.reshape(2, CHG, FRAMES, FFTLEN)
    transform = jnp.fft.fft(framed[0] + 1j * framed[1], axis=-1) * (1.0 / math.sqrt(FFTLEN))
    parts = jnp.stack([jnp.real(transform), jnp.imag(transform)]).astype(jnp.float32)
    digits = parts.reshape(2, CHG, FRAMES, FFT_HI, FFT_LO)
    return jnp.swapaxes(digits, -1, -2)

def reference(strengths, sample_cell, sample_frac):
    by_group = jnp.moveaxis(strengths, 1, 0)
    result = lax.map(lambda group_strengths: one_group(group_strengths, sample_cell, sample_frac), by_group)
    return jnp.moveaxis(result, 0, 1)
```

```python
import functools
import math

import jax
import jax.numpy as jnp
import numpy as np
from jax import lax
from jax.experimental import pallas as pl
from jax.experimental.pallas import tpu as pltpu
from jax.sharding import PartitionSpec as P


TAPS = 8
GRID_DEV = 1024
FFT_LO = 32
FFT_HI = 128
FFTLEN = 4096
HALF = TAPS // 2
LANES = 128

sharpness = 0.3


def cost(flops, nbytes, trans=0):
    return pl.CostEstimate(flops=flops, bytes_accessed=nbytes, transcendentals=trans)


def tap_values(offset, fraction):
    shifted = offset - fraction
    values = jnp.exp2((shifted * shifted) * (-sharpness * math.log2(math.e)))
    return jnp.where(jnp.abs(offset) < float(HALF), values, 0.0).astype(jnp.bfloat16)


def down(row):
    pieces = [
        jnp.broadcast_to(row[:, i : i + LANES], (LANES, LANES)).T
        for i in range(0, row.shape[1], LANES)
    ]
    return jnp.concatenate(pieces, axis=0)


def edge_kernel(first_ref, cell_ref, frac_ref, rows_ref, left_ref, right_ref, table_ref):
    @pl.when(pl.program_id(0) == 0)
    def _():
        place = lax.broadcasted_iota(jnp.int32, table_ref.shape, 0)
        column = jnp.where(place < HALF, place - HALF, place + (GRID_DEV - HALF))
        offset = (column - (cell_ref[...] - first_ref[0])).astype(jnp.float32) - 0.5
        table_ref[...] = tap_values(offset, frac_ref[...] - 0.5)

    rows = rows_ref[...].reshape(-1, rows_ref.shape[-1])
    sums = lax.dot_general(
        table_ref[...], rows, (((1,), (1,)), ((), ())), preferred_element_type=jnp.float32
    )
    left_ref[...] = sums[:HALF]
    right_ref[...] = sums[HALF:TAPS]


def edge_sums(strengths, first, cell_row, frac_row):
    parts, groups, channels, samples = strengths.shape
    some = 2 if groups % 2 == 0 else 1
    blocks = groups // some
    out = jax.ShapeDtypeStruct((HALF, parts * groups * channels), jnp.float32)
    return pl.pallas_call(
        edge_kernel,
        grid_spec=pltpu.PrefetchScalarGridSpec(
            num_scalar_prefetch=1,
            grid=(parts * blocks,),
            in_specs=[
                pl.BlockSpec((1, samples), lambda i, at: (0, 0)),
                pl.BlockSpec((1, samples), lambda i, at: (0, 0)),
                pl.BlockSpec(
                    (1, some, channels, samples), lambda i, at: (i // blocks, i % blocks, 0, 0)
                ),
            ],
            out_specs=[pl.BlockSpec((HALF, some * channels), lambda i, at: (0, i))] * 2,
            scratch_shapes=[pltpu.VMEM((2 * TAPS, samples), jnp.bfloat16)],
        ),
        out_shape=[out] * 2,
        cost_estimate=cost(2 * 256 * strengths.size, 2 * strengths.size),
        name="edge_sums",
    )(first, cell_row, frac_row, strengths)


def table_kernel(first_ref, cell_ref, frac_ref, out_ref):
    lane = lax.broadcasted_iota(jnp.int32, (LANES, LANES), 1).astype(jnp.float32)
    cells = (cell_ref[...] - first_ref[0]).astype(jnp.float32) + 0.5
    fractions = frac_ref[...] - 0.5
    for i in range(0, out_ref.shape[0], LANES):
        base = lane - down(cells[:, i : i + LANES])
        fraction = down(fractions[:, i : i + LANES])
        for j in range(0, out_ref.shape[1], LANES):
            out_ref[i : i + LANES, j : j + LANES] = tap_values(base + float(j), fraction)


def tap_table(first, cell_row, frac_row):
    samples = cell_row.shape[1]
    block = min(512, samples)
    return pl.pallas_call(
        table_kernel,
        grid_spec=pltpu.PrefetchScalarGridSpec(
            num_scalar_prefetch=1,
            grid=(samples // block,),
            in_specs=[
                pl.BlockSpec((1, block), lambda i, at: (0, i)),
                pl.BlockSpec((1, block), lambda i, at: (0, i)),
            ],
            out_specs=pl.BlockSpec((block, GRID_DEV), lambda i, at: (i, 0)),
        ),
        out_shape=jax.ShapeDtypeStruct((samples, GRID_DEV), jnp.bfloat16),
        cost_estimate=cost(
            20 * samples * GRID_DEV, 2 * samples * GRID_DEV, samples * GRID_DEV
        ),
        name="tap_table",
    )(first, cell_row, frac_row)


def spread_kernel(zones, pos_ref, table_ref, rows_ref, *refs):
    parts, groups, channels, samples = rows_ref.shape
    halo_refs, out_refs, sums_ref = refs[: 2 * parts], refs[2 * parts : -1], refs[-1]
    width = table_ref.shape[1]
    step = pl.program_id(0)
    rows = rows_ref[...].reshape(parts * groups * channels, samples)
    sums = jnp.dot(rows, table_ref[...], preferred_element_type=jnp.float32)
    sums_ref[...] = sums.reshape(sums_ref.shape)

    def add_halo(refs, lanes, last):
        for part, ref in enumerate(refs):
            edge = ref[...]
            fill = jnp.zeros((LANES - HALF, edge.shape[1]), jnp.float32)
            turned = jnp.concatenate([fill, edge] if last else [edge, fill], axis=0).T
            sums_ref[part, :, :, lanes] += turned.reshape(groups, channels, LANES)

    @pl.when(step == 0)
    def _():
        add_halo(halo_refs[:parts], slice(0, LANES), False)

    @pl.when(step == pl.num_programs(0) - 1)
    def _():
        add_halo(halo_refs[parts:], slice(width - LANES, width), True)

    here = channels // zones
    for k in range(zones):
        base = pl.multiple_of((pos_ref[0] ^ k) * here, here)
        for part in range(parts):
            for group in range(groups):
                block = sums_ref[part, group, pl.ds(base, here), :].astype(jnp.bfloat16)
                if len(out_refs) == 1:
                    squad, _, _, _, per, _ = out_refs[0].shape
                    out_refs[0][:, k, group, part] = block.reshape(squad, per, width)
                else:
                    squad, _, _, per, _ = out_refs[k].shape
                    out_refs[k][:, group, part] = block.reshape(squad, per, width)


def spread(strengths, halo, table, position, first, count, zones, squad, merged):
    parts, groups, channels, samples = strengths.shape
    per = channels // zones // squad
    width = min(512, GRID_DEV)
    at = first // count
    if merged:
        shape = (squad, zones, count, parts, per)
        copies = 1
    else:
        shape = (squad, count, parts, per)
        copies = zones
    out = jax.ShapeDtypeStruct((*shape, GRID_DEV), jnp.bfloat16)
    lead = (0,) * len(shape)
    blocks = groups // count
    halo_specs = [
        pl.BlockSpec((HALF, count * channels), lambda n, pos, p=p: (0, p * blocks + at))
        for p in range(parts)
    ]
    return pl.pallas_call(
        functools.partial(spread_kernel, zones),
        grid_spec=pltpu.PrefetchScalarGridSpec(
            num_scalar_prefetch=1,
            grid=(GRID_DEV // width,),
            in_specs=[
                pl.BlockSpec((samples, width), lambda n, pos: (0, n)),
                pl.BlockSpec((parts, count, channels, samples), lambda n, pos: (0, at, 0, 0)),
                *halo_specs,
                *halo_specs,
            ],
            out_specs=[pl.BlockSpec((*shape, width), lambda n, pos: (*lead, n))] * copies,
            scratch_shapes=[pltpu.VMEM((parts, count, channels, width), jnp.float32)],
        ),
        out_shape=[out] * copies,
        cost_estimate=cost(
            2 * parts * count * channels * samples * GRID_DEV,
            2 * parts * count * channels * (samples + GRID_DEV),
        ),
        name="spread",
    )(position, table, strengths, *[halo[0]] * parts, *[halo[1]] * parts)


def transform_kernel(frames, pos_ref, d_hi, d_lo, h_ref, twist_ref, *refs):
    in_refs = refs[:frames]
    out_ref, x_ref = refs[-2:]
    squad, groups, parts, per, cells = in_refs[0].shape
    inner = cells // FFT_HI
    row = 0
    for step in range(squad):
        for part in range(parts):
            for x in range(inner):
                for g in range(groups):
                    for m in range(frames):
                        lane = (g * frames + m) * FFT_HI
                        x_ref[row : row + per, lane : lane + FFT_HI] = in_refs[m][
                            step, g, part, :, x * FFT_HI : (x + 1) * FFT_HI
                        ]
                row += per
    half = per * FFT_LO
    signal = x_ref[...]
    first = jnp.dot(d_hi[...], signal, preferred_element_type=jnp.float32) + jnp.dot(
        d_lo[...], signal, preferred_element_type=jnp.float32
    )
    cosine = twist_ref[0]
    sine = twist_ref[1]
    for g in range(groups):
        for m in range(frames):
            lane = (g * frames + m) * FFT_HI
            piece = first[:, lane : lane + FFT_HI].reshape(2, per, FFT_LO, FFT_HI)
            real = piece[0] * cosine + piece[1] * sine
            imag = piece[1] * cosine - piece[0] * sine
            turned = jnp.concatenate(
                [real.reshape(half, FFT_HI), imag.reshape(half, FFT_HI)], axis=1
            )
            high = turned.astype(jnp.bfloat16)
            low = (turned - high.astype(jnp.float32)).astype(jnp.bfloat16)
            result = jnp.dot(
                jnp.concatenate([high, low], axis=1),
                h_ref[...],
                preferred_element_type=jnp.float32,
            )
            result = result[:, : 2 * FFT_HI] + result[:, 2 * FFT_HI :]
            for part in range(2):
                out_ref[part, g, :, pos_ref[1] ^ m] = result[
                    :, part * FFT_HI : (part + 1) * FFT_HI
                ].reshape(per, FFT_LO, FFT_HI)


def transform(received, spectra, tables, position, sides, total_groups, first):
    frames = sides[1]
    if received[0].ndim == 6:
        squad, zones, count, parts, per, cells = received[0].shape
        kinds = zones // frames
    else:
        squad, count, parts, per, cells = received[0].shape
        kinds = 1
    some = 2 if count % 2 == 0 else 1
    groups = total_groups // sides[0]
    block = (squad, some, parts, per, cells)
    if received[0].ndim == 6:
        data_specs = [
            pl.BlockSpec(
                (squad, None, some, parts, per, cells),
                lambda k, i, pos, m=m: (0, k * frames + m, i, 0, 0, 0),
            )
            for m in range(frames)
        ]
        data = [received[0]] * frames
    else:
        data_specs = [pl.BlockSpec(block, lambda k, i, pos: (0, i, 0, 0, 0))] * frames
        data = list(received)
    in_specs = [pl.BlockSpec(memory_space=pltpu.VMEM)] * 4 + data_specs
    operands = [*tables, *data]
    aliases = {}
    if spectra is not None:
        in_specs.append(pl.BlockSpec(memory_space=pl.ANY))
        operands.append(spectra)
        aliases = {len(operands): 0}
    rows = 2 * FFT_LO * per
    return pl.pallas_call(
        functools.partial(transform_kernel, frames),
        grid_spec=pltpu.PrefetchScalarGridSpec(
            num_scalar_prefetch=1,
            grid=(kinds, count // some),
            in_specs=in_specs,
            out_specs=pl.BlockSpec(
                (2, some, per, frames, FFT_LO, FFT_HI),
                lambda k, i, pos: (0, ((pos[0] ^ k) * groups + first) // some + i, 0, 0, 0, 0),
            ),
            scratch_shapes=[pltpu.VMEM((rows, some * frames * FFT_HI), jnp.bfloat16)],
        ),
        out_shape=jax.ShapeDtypeStruct(
            (2, total_groups, per, frames, FFT_LO, FFT_HI), jnp.float32
        ),
        input_output_aliases=aliases,
        cost_estimate=cost(
            4 * kinds * count * rows * rows * frames * FFT_HI, 12 * kinds * count * rows * FFT_HI
        ),
        name="transform",
    )(position, *operands)


def split_bf16(values):
    values = np.asarray(values, np.float32)
    high = values.astype(jnp.bfloat16)
    low = (values - high.astype(np.float32)).astype(jnp.bfloat16)
    return high, low


def transform_tables(per):
    low = np.arange(FFT_LO)
    high = np.arange(FFT_HI)
    angle = 2.0 * math.pi / FFT_LO * (np.outer(low, low) % FFT_LO)
    c, s = np.cos(angle), np.sin(angle)
    inner = GRID_DEV // FFT_HI
    steps = FFT_LO // inner
    small = np.block([[c, s], [-s, c]])
    small = small.reshape(2 * FFT_LO, 2, steps, inner).transpose(0, 2, 1, 3)
    small = small.reshape(2 * FFT_LO, 2 * FFT_LO)
    size = 2 * FFT_LO * per
    row = lax.broadcasted_iota(jnp.int32, (size, size), 0)
    column = lax.broadcasted_iota(jnp.int32, (size, size), 1)
    same = (row // FFT_LO) % per == column % per
    tall_row = lax.broadcasted_iota(jnp.int32, (size, 2 * FFT_LO), 0)
    tall_col = lax.broadcasted_iota(jnp.int32, (size, 2 * FFT_LO), 1)
    pick_row = tall_row // (FFT_LO * per) * FFT_LO + tall_row % FFT_LO == tall_col
    wide_row = lax.broadcasted_iota(jnp.int32, (2 * FFT_LO, size), 0)
    wide_col = lax.broadcasted_iota(jnp.int32, (2 * FFT_LO, size), 1)
    pick_col = wide_col // per == wide_row

    def widen(piece):
        tall = jnp.dot(
            pick_row.astype(jnp.bfloat16), jnp.asarray(piece), preferred_element_type=jnp.float32
        ).astype(jnp.bfloat16)
        big = jnp.dot(tall, pick_col.astype(jnp.bfloat16), preferred_element_type=jnp.float32)
        return jnp.where(same, big, 0.0).astype(jnp.bfloat16)

    d_hi, d_lo = (widen(piece) for piece in split_bf16(small))
    angle = 2.0 * math.pi / FFT_HI * (np.outer(high, high) % FFT_HI)
    c, s = np.cos(angle), np.sin(angle)
    h_hi, h_lo = split_bf16(np.block([[c, -s], [s, c]]) / math.sqrt(FFTLEN))
    second = np.block([[h_hi, h_lo], [h_hi, np.zeros_like(h_lo)]])
    angle = 2.0 * math.pi / FFTLEN * np.outer(low, high)
    twist = np.stack([np.cos(angle), np.sin(angle)])
    return d_hi, d_lo, jnp.asarray(second), jnp.asarray(twist.astype(np.float32))


def shards(strengths, sample_cell, sample_frac):
    time_count = lax.axis_size("tm")
    sides = lax.axis_size("freq")
    squad = FFTLEN // GRID_DEV
    zones = time_count // squad
    frames = zones // sides
    _, groups, channels, _ = strengths.shape
    me = lax.axis_index("tm").astype(jnp.int32)
    side = lax.axis_index("freq").astype(jnp.int32)
    zone = me // squad

    first_cell = (me * GRID_DEV)[None]
    cell = sample_cell[None, :]
    fraction = sample_frac[None, :]
    to_left, to_right = edge_sums(strengths, first_cell, cell, fraction)
    ring = [(i, (i + 1) % time_count) for i in range(time_count)]
    back = [(j, i) for i, j in ring]
    halo = (lax.ppermute(to_right, "tm", ring), lax.ppermute(to_left, "tm", back))
    table = tap_table(first_cell, cell, fraction)
    tables = transform_tables(channels // time_count)
    start = (zone % frames + frames * side)[None]
    place = jnp.stack([zone // frames, zone % frames])

    def hop(k):
        pairs = []
        for t in range(time_count):
            for f in range(sides):
                z, r = divmod(t, squad)
                far = (z % frames + frames * f) ^ k
                pairs.append((t * sides + f, (far * squad + r) * sides + z // frames))
        return pairs

    squads = [[z * squad + i for i in range(squad)] for z in range(zones)]

    def cross(block, k):
        return lax.ppermute(block, ("tm", "freq"), hop(k))

    def share(block):
        return lax.all_to_all(
            block, "tm", split_axis=0, concat_axis=0, axis_index_groups=squads, tiled=True
        )

    count = max(1, groups // 2)
    early = groups - count
    spectra = None
    later = []
    if early:
        blocks = spread(strengths, halo, table, start, 0, early, zones, squad, False)
        crossed = [cross(blocks[k], k) for k in range(zones)]
    (block,) = spread(strengths, halo, table, start, early, count, zones, squad, True)
    shared = share(block)
    pieces = [shared[:, k] for k in range(zones)]
    later = [cross(pieces[k], k) for k in range(zones)]
    shape = ((sides, frames), sides * groups)
    if early:
        joined = jnp.stack(crossed, axis=1)
        gathered = share(joined)
        spectra = transform([gathered], None, tables, place, *shape, 0)
    for kind in range(sides):
        at = place ^ jnp.array([kind, 0], jnp.int32)
        mine = later[kind * frames : (kind + 1) * frames]
        spectra = transform(mine, spectra, tables, at, *shape, early)
    return spectra


def solution(mesh):
    placed = (P(None, "freq", None, "tm"), P("tm"), P("tm"))
    return jax.shard_map(
        shards,
        mesh=mesh,
        in_specs=placed,
        out_specs=P(None, None, "tm", "freq", None, None),
        check_vma=False,
    )
```
